32 devices in a mesh: dom: 32 (over z, y, x, core).
Axes of the slice: x: 2, y: 2, z: 4, core: 2. Of those that a mesh axis runs over, the one named last changes fastest.
Arguments:
- features: bfloat16 [131072, 256], P('dom'), may hold values from -6 to 6
- weight: bfloat16 [256, 256], replicated, may hold values from -0.375 to 0.375
- bias_vector: float32 [256], replicated, may hold values from -3 to 3
- tile_values: bfloat16 [8192, 128, 128], P('dom'), may hold values from -0.1875 to 0.1875
- tile_row: int32 [32, 256], P('dom'), may hold values from 0 to 31
- tile_col: int32 [32, 256], P('dom'), may hold values from 0 to 35
- tile_count: int32 [32], P('dom'), may hold values from 64 to 256, as said below
- send_rows: int32 [32, 32, 16], P('dom'), may hold values from 0 to 4095, as said below
- send_count: int32 [32, 32], P('dom'), may hold values from 0 to 16, as said below
- cotangent: bfloat16 [131072, 256], P('dom'), may hold values from -6 to 6
Outputs:
- activation: bfloat16 [131072, 256], P('dom')
- grad_features: bfloat16 [131072, 256], P('dom')
- grad_weight: float32 [256, 256], replicated
- grad_bias: float32 [256], replicated
The draws below stay inside these ranges and needn't reach their ends.
Inputs may be any that keep to these rules, and one draw needn't show every extreme that they name: `tile_count`: each partition uses at least a quarter of its slots; in every draw two partitions use all 256. `send_rows`: for each sender and reader the 16 listed rows are distinct. `send_count`: in every draw one reader receives 16 rows from every partition.
All inputs are finite; a program needn't handle non-finite values.
Results may differ from the reference program's by a relative error of at most 0.0061.
Values may be sent and summed in bfloat16 or wider, within the bound.
A program may use at most 192 MiB of HBM per device.

```python
import jax
import jax.numpy as jnp
from jax import lax

F = 256
TB = 128
TPB = 8
SLOT = 16
ROWS_DEV = 4096
NB = 32
KMAX = 256
EB = 36
NODES = 131072
N_DOM = 32


def draw_tile_count(key, part):
    first_key, second_key = jax.random.split(jax.random.fold_in(key, 5))
    base_counts = jax.random.randint(first_key, (N_DOM,), KMAX // 4, KMAX // 2 + 1)
    shuffled = jax.random.permutation(second_key, N_DOM)
    return jnp.where(shuffled < 2, KMAX, base_counts).astype(jnp.int32)


def draw_send_rows(key, part):
    first_key, second_key = jax.random.split(jax.random.fold_in(key, 11))
    beginning = jax.random.randint(first_key, (N_DOM, N_DOM, 1), 0, ROWS_DEV)
    increments = jax.random.randint(second_key, (N_DOM, N_DOM, SLOT), 1, ROWS_DEV // SLOT + 1)
    increments = increments.at[:, :, 0].set(0)
    return ((beginning + jnp.cumsum(increments, axis=2)) % ROWS_DEV).astype(jnp.int32)


def draw_send_count(key, part):
    first_key, second_key = jax.random.split(jax.random.fold_in(key, 23))
    counts_drawn = jax.random.randint(first_key, (N_DOM, N_DOM), 0, SLOT + 1)
    full_reader = jax.random.randint(second_key, (), 0, N_DOM)
    column_ids = lax.broadcasted_iota(jnp.int32, (N_DOM, N_DOM), 1)
    return jnp.where(column_ids == full_reader, SLOT, counts_drawn).astype(jnp.int32)


def touch_ends(values, own_key, smallest, high):
    spot = [jax.random.randint(jax.random.fold_in(own_key, axis), (), 0, length) for axis, length in enumerate(values.shape)]
    longest = values.shape.index(max(values.shape))
    beside = spot[:longest] + [(spot[longest] + 1) % values.shape[longest]] + spot[longest + 1:]
    return values.at[tuple(spot)].set(smallest).at[tuple(beside)].set(high)


def shard_levels(key, dims, pieces, low, largest):
    level = 1.0
    for dim, blocks in pieces:
        steps = jax.random.uniform(jax.random.fold_in(jax.random.fold_in(key, 6), dim), (blocks,), jnp.float32, low / len(pieces), largest / len(pieces))
        level = level * jnp.repeat(jnp.exp(steps), dims[dim] // blocks).reshape((-1,) + (1,) * (len(dims) - 1 - dim))
    return level


def gaussian(stream_key, dims, deviation, bound, cuts=(), kind=jnp.bfloat16):
    values = jax.random.normal(stream_key, dims, jnp.float32) * deviation
    if len(cuts) > 0:
        values = shard_levels(stream_key, dims, cuts, -0.22, 0.18) * values
    return jnp.clip(values, min=-bound, max=bound).astype(kind)


def setup_inputs(seed: int = 0) -> dict:
    keys = jax.random.split(jax.random.key(seed), 11)
    features = gaussian(keys[0], (NODES, F), 1.0, 6.0, ((0, 32),))
    weight = gaussian(keys[1], (F, F), F ** -0.5, 0.375)
    bias_vector = gaussian(keys[2], (F,), 0.5, 3.0, (), jnp.float32)
    tile_values = gaussian(keys[3], (N_DOM * KMAX, TB, TB), (TB * TPB) ** -0.5, 0.1875, ((0, 32),))
    tile_row = touch_ends(jax.random.randint(keys[4], (N_DOM, KMAX), 0, NB), jax.random.fold_in(keys[4], 1), 0, NB - 1).astype(jnp.int32)
    tile_col = touch_ends(jax.random.randint(keys[5], (N_DOM, KMAX), 0, EB), jax.random.fold_in(keys[5], 1), 0, EB - 1).astype(jnp.int32)
    tile_count = draw_tile_count(jax.random.fold_in(keys[10], 71), 0)
    send_rows = draw_send_rows(jax.random.fold_in(keys[10], 71), 0)
    send_count = draw_send_count(jax.random.fold_in(keys[10], 71), 0)
    cotangent = gaussian(keys[9], (NODES, F), 1.0, 6.0, ((0, 32),))
    return dict(features=features, weight=weight, bias_vector=bias_vector, tile_values=tile_values, tile_row=tile_row, tile_col=tile_col, tile_count=tile_count, send_rows=send_rows, send_count=send_count, cotangent=cotangent)


def reference(features, weight, bias_vector, tile_values, tile_row, tile_col, tile_count, send_rows, send_count, cotangent):
    feature_width = features.shape[1]
    feature_parts = features.reshape(N_DOM, ROWS_DEV, feature_width)
    tile_parts = tile_values.reshape(N_DOM, KMAX, TB, TB)
    slot_index = jnp.arange(SLOT, dtype=jnp.int32)
    live_slots = slot_index[None, None, :] < send_count[:, :, None]
    device_ids = jnp.arange(N_DOM, dtype=jnp.int32)
    tile_ids = jnp.arange(KMAX, dtype=jnp.int32)

    def outgoing(owner_index):
        picked = feature_parts[owner_index][send_rows[owner_index]]
        return jnp.where(live_slots[owner_index][:, :, None], picked, jnp.zeros_like(picked))

    outbound = lax.map(outgoing, device_ids)
    halo_rows = jnp.swapaxes(outbound, 0, 1)

    def forward(reader_index):
        extended = jnp.concatenate([feature_parts[reader_index], halo_rows[reader_index].reshape(N_DOM * SLOT, feature_width)], 0)
        ext_blocks = extended.reshape(EB, TB, feature_width)
        fetched = ext_blocks[tile_col[reader_index]].astype(jnp.float32)
        products = jnp.einsum("kij,kjf->kif", tile_parts[reader_index].astype(jnp.float32), fetched, precision=lax.Precision.HIGHEST)
        selected = tile_ids < tile_count[reader_index]
        levels = jnp.arange(NB, dtype=jnp.int32)
        one_hot = ((tile_row[reader_index][None, :] == levels[:, None]) & selected[None, :]).astype(jnp.float32)
        summed = jnp.dot(one_hot, products.reshape(KMAX, -1), precision=lax.Precision.HIGHEST)
        return summed.reshape(ROWS_DEV, feature_width).astype(jnp.bfloat16)

    aggregated = lax.map(forward, device_ids).reshape(NODES, feature_width)
    linear = jnp.dot(aggregated, weight, preferred_element_type=jnp.float32) + bias_vector
    sigmoid_value = jax.nn.sigmoid(linear)
    activation = (linear * sigmoid_value).astype(jnp.bfloat16)
    slope_value = sigmoid_value * (1.0 + linear * (1.0 - sigmoid_value))
    grad_linear = (cotangent.astype(jnp.float32) * slope_value).astype(jnp.bfloat16)
    norm_scale = NODES ** -0.5
    grad_weight = jnp.dot(aggregated.T, grad_linear, preferred_element_type=jnp.float32) * norm_scale
    grad_bias = jnp.sum(grad_linear.astype(jnp.float32), axis=0) * norm_scale
    grad_mixed = jnp.dot(grad_linear, weight.T, preferred_element_type=jnp.float32).astype(jnp.bfloat16)
    mixed_parts = grad_mixed.reshape(N_DOM, NB, TB, feature_width)

    def backward(reader_index):
        fetched = mixed_parts[reader_index][tile_row[reader_index]].astype(jnp.float32)
        products = jnp.einsum("kji,kjf->kif", tile_parts[reader_index].astype(jnp.float32), fetched, precision=lax.Precision.HIGHEST)
        selected = tile_ids < tile_count[reader_index]
        levels = jnp.arange(EB, dtype=jnp.int32)
        one_hot = ((tile_col[reader_index][None, :] == levels[:, None]) & selected[None, :]).astype(jnp.float32)
        summed = jnp.dot(one_hot, products.reshape(KMAX, -1), precision=lax.Precision.HIGHEST)
        summed = summed.reshape(EB * TB, feature_width)
        own_part = summed[:ROWS_DEV]
        halo_part = summed[ROWS_DEV:].astype(jnp.bfloat16).reshape(N_DOM, SLOT, feature_width)
        return own_part, halo_part

    own_grad, halo_grad = lax.map(backward, device_ids)

    def collect(owner_index):
        incoming = halo_grad[:, owner_index].astype(jnp.float32)
        incoming = jnp.where(live_slots[owner_index][:, :, None], incoming, jnp.zeros_like(incoming))
        return jax.ops.segment_sum(incoming.reshape(-1, feature_width), send_rows[owner_index].reshape(-1), num_segments=ROWS_DEV)

    collected = lax.map(collect, device_ids)
    grad_features = (own_grad + collected).reshape(NODES, feature_width).astype(jnp.bfloat16)
    return (activation, grad_features, grad_weight, grad_bias)
```

```python
import functools
import math

import jax
import jax.numpy as jnp
from jax import lax
from jax.experimental import pallas as pl
from jax.experimental.pallas import tpu as pltpu
from jax.sharding import PartitionSpec as P

MESH = pl.DeviceIdType.MESH
VMEM = pltpu.VMEM
f32 = jnp.float32
bf16 = jnp.bfloat16


def greet(n, me):
    barrier = pltpu.get_barrier_semaphore()

    def signal(i, carry):
        pl.semaphore_signal(
            barrier, inc=1, device_id=(lax.rem(me + i, n),), device_id_type=MESH
        )
        return carry

    lax.fori_loop(1, n, signal, 0)
    return barrier


def push(n, me, src, dst, send_sem, recv_sem, i):
    peer = lax.rem(me + i, n)
    return pltpu.make_async_remote_copy(
        src_ref=src(peer),
        dst_ref=dst.at[me],
        send_sem=send_sem.at[i],
        recv_sem=recv_sem.at[i],
        device_id=(peer,),
        device_id_type=MESH,
    )


def gather_kernel(n, chosen_ref, features_ref, halo_ref, total, sent, landed, send_sem, recv_sem):
    me = lax.axis_index("dom")
    barrier = greet(n, me)
    slots = chosen_ref.shape[0]
    rows = features_ref.shape[0]
    step = math.gcd(rows, 512)
    for c in range(rows // step):
        ids = lax.broadcasted_iota(jnp.int32, (slots, step), 1) + c * step
        hot = jnp.where(ids == chosen_ref[...], 1.0, 0.0).astype(bf16)
        part = jnp.dot(hot, features_ref[pl.ds(c * step, step), :], preferred_element_type=f32)
        if c == 0:
            total[...] = part
        else:
            total[...] += part
    sent[...] = total[...].astype(bf16).reshape(sent.shape)
    pl.semaphore_wait(barrier, n - 1)
    copy = functools.partial(push, n, me, lambda p: sent.at[p], landed, send_sem, recv_sem)

    def start(i, carry):
        copy(i).start()
        return carry

    def finish(i, carry):
        copy(i).wait()
        return carry

    lax.fori_loop(1, n, start, 0)
    landed[me] = sent[me]
    lax.fori_loop(1, n, finish, 0)
    halo_ref[...] = landed[...]


def exchange_gather(n, chosen, features, slot_count):
    width = features.shape[1]
    slots = chosen.shape[0]
    block = (n, slot_count, width)
    return pl.pallas_call(
        functools.partial(gather_kernel, n),
        out_shape=jax.ShapeDtypeStruct(block, bf16),
        in_specs=[pl.BlockSpec(memory_space=VMEM)] * 2,
        out_specs=pl.BlockSpec(memory_space=VMEM),
        scratch_shapes=[
            VMEM((slots, width), f32),
            VMEM(block, bf16),
            VMEM(block, bf16),
            pltpu.SemaphoreType.DMA((n,)),
            pltpu.SemaphoreType.DMA((n,)),
        ],
        compiler_params=pltpu.CompilerParams(collective_id=0, has_side_effects=True),
        name="gather_exchange",
    )(chosen, features)


GROUP = 8
CHUNK = 16


def local_kernel(
    tile_row, tile_col, tile_count, features, halo, tiles, cotangent, weight, bias,
    activation, own_grad, halo_grad, weight_part, bias_part,
    source, held, cot, act, mixed, forward, backward, spread, wsum, bsum,
    in_sem, tile_sem, cot_sem, act_sem, out_sem,
):
    own = features.shape[0]
    ext = own + halo.shape[0]
    number = tiles.shape[0]
    chunk = math.gcd(number, CHUNK)
    group = math.gcd(chunk, GROUP)
    total = tile_count[0]
    chunks = (total + chunk - 1) // chunk

    def tile_copy(c):
        span = pl.ds(c * chunk, chunk)
        return pltpu.make_async_copy(tiles.at[span], held.at[span], tile_sem.at[c])

    copies = [
        pltpu.make_async_copy(features, source.at[pl.ds(0, own)], in_sem.at[0]),
        pltpu.make_async_copy(halo, source.at[pl.ds(own, ext - own)], in_sem.at[1]),
    ]
    for copy in copies:
        copy.start()

    @pl.loop(0, chunks)
    def _(c):
        tile_copy(c).start()

    cot_copy = pltpu.make_async_copy(cotangent, cot, cot_sem)
    cot_copy.start()

    @pl.loop(0, own)
    def _(r):
        forward[r] = jnp.zeros(forward.shape[1:], f32)
        backward[r] = jnp.zeros(backward.shape[1:], f32)

    for r in range(own, ext):
        backward[r] = jnp.zeros(backward.shape[1:], f32)
    for copy in copies:
        copy.wait()

    @pl.loop(0, chunks)
    def _(c):
        tile_copy(c).wait()
        for g in range(chunk // group):
            base = c * chunk + g * group
            for j in range(group):
                k = base + j
                product = jnp.dot(held[k], source[tile_col[0, k]], preferred_element_type=f32)
                target = jnp.where(k < total, tile_row[0, k], own)
                forward[target] += product

    cot_copy.wait()
    edge = tiles.shape[1]
    step = math.gcd(own, 4)
    width = weight.shape[0]
    wsum[...] = jnp.zeros_like(wsum)
    bsum[...] = jnp.zeros_like(bsum)

    def act_copy(b):
        span = pl.ds(b * step, step)
        return pltpu.make_async_copy(act.at[span], activation.at[span], act_sem.at[b])

    @pl.loop(0, own // step)
    def _(b):
        span = pl.ds(b * step, step)
        agg = forward[span].astype(bf16).reshape(step * edge, width)
        linear = jnp.dot(agg, weight[...], preferred_element_type=f32) + bias[...]
        sig = jax.nn.sigmoid(linear)
        act[span] = (linear * sig).astype(bf16).reshape(step, edge, width)
        act_copy(b).start()
        slope = sig * (1.0 + linear * (1.0 - sig))
        grad = (cot[span].reshape(step * edge, width).astype(f32) * slope).astype(bf16)
        wsum[...] += lax.dot_general(
            agg, grad, (((0,), (0,)), ((), ())), preferred_element_type=f32
        )
        bsum[...] += jnp.sum(grad.astype(f32), axis=0, keepdims=True)
        back = lax.dot_general(
            grad, weight[...], (((1,), (1,)), ((), ())), preferred_element_type=f32
        )
        mixed[span] = back.astype(bf16).reshape(step, edge, width)

    @pl.loop(0, chunks * (chunk // group))
    def _(g):
        for j in range(group):
            k = g * group + j
            product = lax.dot_general(
                held[k], mixed[tile_row[0, k]], (((0,), (0,)), ((), ())),
                preferred_element_type=f32,
            )
            target = jnp.where(k < total, tile_col[0, k], ext)
            backward[target] += product

    def out_copy(b):
        span = pl.ds(b * step, step)
        return pltpu.make_async_copy(spread.at[span], own_grad.at[span], out_sem.at[b])

    @pl.loop(0, own // step)
    def _(b):
        span = pl.ds(b * step, step)
        spread[span] = backward[span].astype(bf16)
        out_copy(b).start()

    halo_grad[...] = backward[pl.ds(own, ext - own)].astype(bf16)
    pieces, piece_rows = weight_part.shape[:2]
    for p in range(pieces):
        weight_part[p] = wsum[pl.ds(p * piece_rows, piece_rows), :].astype(bf16)
    bias_part[...] = bsum[...]

    @pl.loop(0, own // step)
    def _(b):
        act_copy(b).wait()
        out_copy(b).wait()


def local_pass(n, tile_row, tile_col, tile_count, features, halo, tiles, cotangent, weight, bias):
    own, edge, width = features.shape
    ext = own + halo.shape[0]
    number = tiles.shape[0]
    chunk = math.gcd(number, CHUNK)
    steps = own // math.gcd(own, 4)
    anywhere = pl.BlockSpec(memory_space=pltpu.HBM)
    smem = pl.BlockSpec(memory_space=pltpu.SMEM)
    vmem = pl.BlockSpec(memory_space=VMEM)
    dma = pltpu.SemaphoreType.DMA
    return pl.pallas_call(
        local_kernel,
        out_shape=(
            jax.ShapeDtypeStruct(features.shape, bf16),
            jax.ShapeDtypeStruct(features.shape, bf16),
            jax.ShapeDtypeStruct(halo.shape, bf16),
            jax.ShapeDtypeStruct((n, width // n, width), bf16),
            jax.ShapeDtypeStruct((1, width), f32),
        ),
        in_specs=[smem] * 3 + [anywhere] * 4 + [vmem] * 2,
        out_specs=(anywhere, anywhere, vmem, vmem, vmem),
        scratch_shapes=[
            VMEM((ext, edge, width), bf16),
            VMEM(tiles.shape, bf16),
            VMEM(features.shape, bf16),
            VMEM(features.shape, bf16),
            VMEM(features.shape, bf16),
            VMEM((own + 1, edge, width), f32),
            VMEM((ext + 1, edge, width), f32),
            VMEM(features.shape, bf16),
            VMEM((width, width), f32),
            VMEM((1, width), f32),
            dma((2,)),
            dma((number // chunk,)),
            dma,
            dma((steps,)),
            dma((steps,)),
        ],
        compiler_params=pltpu.CompilerParams(vmem_limit_bytes=56 * 1024 * 1024),
        name="local_pass",
    )(tile_row, tile_col, tile_count, features, halo, tiles, cotangent, weight, bias)


def return_kernel(
    n, scale, halo_ref, weight_ref, bias_ref, returned_ref, wsum_ref, bsum_ref,
    halo_in, weight_in, bias_in, piece, pieces_in,
    halo_s, halo_r, weight_s, weight_r, bias_s, bias_r, piece_s, piece_r,
):
    me = lax.axis_index("dom")
    barrier = greet(n, me)
    pl.semaphore_wait(barrier, n - 1)
    halo_copy = functools.partial(push, n, me, lambda p: halo_ref.at[p], halo_in, halo_s, halo_r)
    weight_copy = functools.partial(
        push, n, me, lambda p: weight_ref.at[p], weight_in, weight_s, weight_r
    )
    bias_copy = functools.partial(push, n, me, lambda p: bias_ref, bias_in, bias_s, bias_r)
    piece_copy = functools.partial(push, n, me, lambda p: piece, pieces_in, piece_s, piece_r)

    def over(step):
        def turn(i, carry):
            step(i)
            return carry

        lax.fori_loop(1, n, turn, 0)

    def first(i):
        weight_copy(i).start()
        bias_copy(i).start()

    over(first)
    over(lambda i: halo_copy(i).start())
    weight_in[me] = weight_ref[me]
    bias_in[me] = bias_ref[...]
    halo_in[me] = halo_ref[me]
    over(lambda i: weight_copy(i).wait())
    piece[...] = (jnp.sum(weight_in[...].astype(f32), axis=0) * scale).astype(bf16)
    over(lambda i: piece_copy(i).start())
    pieces_in[me] = piece[...]
    over(lambda i: bias_copy(i).wait())
    bsum_ref[...] = jnp.sum(bias_in[...], axis=0) * scale
    over(lambda i: halo_copy(i).wait())
    returned_ref[...] = halo_in[...]
    over(lambda i: piece_copy(i).wait())
    rows = piece.shape[0]
    for p in range(n):
        wsum_ref[pl.ds(p * rows, rows), :] = pieces_in[p].astype(f32)


def exchange_return(n, scale, halo_grad, weight_part, bias_part):
    width = bias_part.shape[1]
    vmem = pl.BlockSpec(memory_space=VMEM)
    return pl.pallas_call(
        functools.partial(return_kernel, n, scale),
        out_shape=(
            jax.ShapeDtypeStruct(halo_grad.shape, bf16),
            jax.ShapeDtypeStruct((width, width), f32),
            jax.ShapeDtypeStruct((1, width), f32),
        ),
        in_specs=[vmem] * 3,
        out_specs=(vmem,) * 3,
        scratch_shapes=[
            VMEM(halo_grad.shape, bf16),
            VMEM(weight_part.shape, bf16),
            VMEM((n,) + bias_part.shape, f32),
            VMEM(weight_part.shape[1:], bf16),
            VMEM(weight_part.shape, bf16),
        ]
        + [pltpu.SemaphoreType.DMA((n,))] * 8,
        compiler_params=pltpu.CompilerParams(collective_id=1, has_side_effects=True),
        name="return_exchange",
    )(halo_grad, weight_part, bias_part)


def scatter_kernel(chosen, returned, own_grad, out):
    rows = out.shape[0]
    base = pl.program_id(0) * rows
    ids = lax.broadcasted_iota(jnp.int32, (rows, chosen.shape[1]), 0) + base
    hot = jnp.where(ids == chosen[...], 1.0, 0.0).astype(bf16)
    collected = jnp.dot(hot, returned[...], preferred_element_type=f32)
    out[...] = (own_grad[...].astype(f32) + collected).astype(bf16)


def scatter_add(chosen, returned, own_grad):
    rows, width = own_grad.shape
    step = math.gcd(rows, 1024)
    whole = lambda i: (0, 0)
    return pl.pallas_call(
        scatter_kernel,
        out_shape=jax.ShapeDtypeStruct(own_grad.shape, bf16),
        grid=(rows // step,),
        in_specs=[
            pl.BlockSpec(chosen.shape, whole),
            pl.BlockSpec(returned.shape, whole),
            pl.BlockSpec((step, width), lambda i: (i, 0)),
        ],
        out_specs=pl.BlockSpec((step, width), lambda i: (i, 0)),
        name="scatter_add",
    )(chosen, returned, own_grad)


def body(
    features, weight, bias_vector, tile_values, tile_row, tile_col, tile_count, send_rows,
    send_count, cotangent,
):
    rows, width = features.shape
    n = lax.axis_size("dom")
    slot_count = send_rows.shape[2]
    edge = tile_values.shape[1]
    own = rows // edge
    slots = n * slot_count
    slot_index = lax.broadcasted_iota(jnp.int32, (n, slot_count), 1)
    chosen = jnp.where(slot_index < send_count[0][:, None], send_rows[0], -1)
    halo = exchange_gather(n, chosen.reshape(slots, 1), features, slot_count)
    blocks = lambda a: a.reshape(-1, edge, width)
    activation, own_grad, halo_grad, weight_part, bias_part = local_pass(
        n, tile_row, tile_col, tile_count, blocks(features), blocks(halo), tile_values,
        blocks(cotangent), weight, bias_vector.reshape(1, width),
    )
    scale = float(rows * n) ** (-0.5)
    returned, weight_sum, bias_sum = exchange_return(
        n, scale, halo_grad.reshape(n, slot_count, width), weight_part, bias_part
    )
    grad_features = scatter_add(
        chosen.reshape(1, slots), returned.reshape(slots, width), own_grad.reshape(rows, width)
    )
    return (activation.reshape(rows, width), grad_features, weight_sum, bias_sum.reshape(width))


def solution(mesh):
    return jax.shard_map(
        body,
        mesh=mesh,
        in_specs=(
            P("dom", None),
            P(),
            P(),
            P("dom", None, None),
            P("dom", None),
            P("dom", None),
            P("dom"),
            P("dom", None, None),
            P("dom", None),
            P("dom", None),
        ),
        out_specs=(P("dom", None), P("dom", None), P(), P()),
        check_vma=False,
    )
```

```python
import functools
import math

import jax
import jax.numpy as jnp
from jax import lax
from jax.experimental import pallas as pl
from jax.experimental.pallas import tpu as pltpu
from jax.sharding import PartitionSpec as P

MESH = pl.DeviceIdType.MESH
VMEM = pltpu.VMEM
f32 = jnp.float32
bf16 = jnp.bfloat16


def greet(n, me):
    barrier = pltpu.get_barrier_semaphore()

    def signal(i, carry):
        pl.semaphore_signal(
            barrier, inc=1, device_id=(lax.rem(me + i, n),), device_id_type=MESH
        )
        return carry

    lax.fori_loop(1, n, signal, 0)
    return barrier


def push(n, me, src, dst, send_sem, recv_sem, i):
    peer = lax.rem(me + i, n)
    return pltpu.make_async_remote_copy(
        src_ref=src(peer),
        dst_ref=dst.at[me],
        send_sem=send_sem.at[i],
        recv_sem=recv_sem.at[i],
        device_id=(peer,),
        device_id_type=MESH,
    )


def live(count_ref, peer, values):
    slot = lax.broadcasted_iota(jnp.int32, values.shape, 0)
    return jnp.where(slot < count_ref[0, peer], values, jnp.zeros_like(values))


def gather_kernel(
    n, count_ref, chosen_ref, features_hbm, halo_ref,
    features_ref, total, sent, landed, send_sem, recv_sem, load_sem,
):
    me = lax.axis_index("dom")
    slots = chosen_ref.shape[0]
    rows = features_ref.shape[0]
    step = math.gcd(rows, 512)
    loads = []
    for c in range(rows // step):
        span = pl.ds(c * step, step)
        loads.append(
            pltpu.make_async_copy(features_hbm.at[span], features_ref.at[span], load_sem.at[c])
        )
        loads[c].start()
    barrier = greet(n, me)
    for c in range(rows // step):
        ids = lax.broadcasted_iota(jnp.int32, (slots, step), 1) + c * step
        hot = jnp.where(ids == chosen_ref[...], 1.0, 0.0).astype(bf16)
        loads[c].wait()
        part = jnp.dot(hot, features_ref[pl.ds(c * step, step), :], preferred_element_type=f32)
        if c == 0:
            total[...] = part
        else:
            total[...] += part
    slot_count = sent.shape[1]
    for p in range(n):
        block = total[pl.ds(p * slot_count, slot_count), :]
        sent[p] = live(count_ref, p, block).astype(bf16)
    pl.semaphore_wait(barrier, n - 1)
    copy = functools.partial(push, n, me, lambda p: sent.at[p], landed, send_sem, recv_sem)

    def start(i, carry):
        copy(i).start()
        return carry

    def finish(i, carry):
        copy(i).wait()
        return carry

    lax.fori_loop(1, n, start, 0)
    landed[me] = sent[me]
    lax.fori_loop(1, n, finish, 0)
    halo_ref[...] = landed[...]


def exchange_gather(n, send_count, chosen, features, slot_count):
    width = features.shape[1]
    slots = chosen.shape[0]
    block = (n, slot_count, width)
    return pl.pallas_call(
        functools.partial(gather_kernel, n),
        out_shape=jax.ShapeDtypeStruct(block, bf16),
        in_specs=[
            pl.BlockSpec(memory_space=pltpu.SMEM),
            pl.BlockSpec(memory_space=VMEM),
            pl.BlockSpec(memory_space=pltpu.HBM),
        ],
        out_specs=pl.BlockSpec(memory_space=VMEM),
        scratch_shapes=[
            VMEM(features.shape, bf16),
            VMEM((slots, width), f32),
            VMEM(block, bf16),
            VMEM(block, bf16),
            pltpu.SemaphoreType.DMA((n,)),
            pltpu.SemaphoreType.DMA((n,)),
            pltpu.SemaphoreType.DMA((features.shape[0] // math.gcd(features.shape[0], 512),)),
        ],
        compiler_params=pltpu.CompilerParams(
            collective_id=0, has_side_effects=True, vmem_limit_bytes=60 * 1024 * 1024
        ),
        cost_estimate=pl.CostEstimate(
            flops=2 * slots * features.shape[0] * width,
            bytes_accessed=16 * features.size,
            transcendentals=0,
        ),
        name="gather_exchange",
    )(send_count, chosen, features)


GROUP = 8
CHUNK = 16


def local_kernel(
    tile_row, tile_col, tile_count, features, halo, tiles, cotangent, weight, bias,
    activation, own_grad, halo_grad, weight_part, bias_part,
    source, held, cot, act, mixed, forward, backward, spread, wsum, bsum,
    in_sem, tile_sem, cot_sem, act_sem, out_sem,
):
    own = features.shape[0]
    ext = own + halo.shape[0]
    number = tiles.shape[0]
    chunk = math.gcd(number, CHUNK)
    group = math.gcd(chunk, GROUP)
    total = tile_count[0]
    chunks = (total + chunk - 1) // chunk

    def tile_copy(c):
        span = pl.ds(c * chunk, chunk)
        return pltpu.make_async_copy(tiles.at[span], held.at[span], tile_sem.at[c])

    copies = [
        pltpu.make_async_copy(features, source.at[pl.ds(0, own)], in_sem.at[0]),
        pltpu.make_async_copy(halo, source.at[pl.ds(own, ext - own)], in_sem.at[1]),
    ]
    for copy in copies:
        copy.start()

    @pl.loop(0, chunks)
    def _(c):
        tile_copy(c).start()

    cot_copy = pltpu.make_async_copy(cotangent, cot, cot_sem)
    cot_copy.start()

    @pl.loop(0, own)
    def _(r):
        forward[r] = jnp.zeros(forward.shape[1:], f32)
        backward[r] = jnp.zeros(backward.shape[1:], f32)

    for r in range(own, ext):
        backward[r] = jnp.zeros(backward.shape[1:], f32)
    for copy in copies:
        copy.wait()

    @pl.loop(0, chunks)
    def _(c):
        tile_copy(c).wait()
        for g in range(chunk // group):
            base = c * chunk + g * group
            for j in range(group):
                k = base + j
                product = jnp.dot(held[k], source[tile_col[0, k]], preferred_element_type=f32)
                target = jnp.where(k < total, tile_row[0, k], own)
                forward[target] += product

    cot_copy.wait()
    edge = tiles.shape[1]
    step = math.gcd(own, 4)
    width = weight.shape[0]
    wsum[...] = jnp.zeros_like(wsum)
    bsum[...] = jnp.zeros_like(bsum)

    def act_copy(b):
        span = pl.ds(b * step, step)
        return pltpu.make_async_copy(act.at[span], activation.at[span], act_sem.at[b])

    @pl.loop(0, own // step)
    def _(b):
        span = pl.ds(b * step, step)
        agg = forward[span].astype(bf16).reshape(step * edge, width)
        linear = jnp.dot(agg, weight[...], preferred_element_type=f32) + bias[...]
        sig = jax.nn.sigmoid(linear)
        act[span] = (linear * sig).astype(bf16).reshape(step, edge, width)
        act_copy(b).start()
        slope = sig * (1.0 + linear * (1.0 - sig))
        grad = (cot[span].reshape(step * edge, width).astype(f32) * slope).astype(bf16)
        wsum[...] += lax.dot_general(
            agg, grad, (((0,), (0,)), ((), ())), preferred_element_type=f32
        )
        bsum[...] += jnp.sum(grad.astype(f32), axis=0, keepdims=True)
        back = lax.dot_general(
            grad, weight[...], (((1,), (1,)), ((), ())), preferred_element_type=f32
        )
        mixed[span] = back.astype(bf16).reshape(step, edge, width)

    @pl.loop(0, chunks * (chunk // group))
    def _(g):
        for j in range(group):
            k = g * group + j
            product = lax.dot_general(
                held[k], mixed[tile_row[0, k]], (((0,), (0,)), ((), ())),
                preferred_element_type=f32,
            )
            target = jnp.where(k < total, tile_col[0, k], ext)
            backward[target] += product

    def out_copy(b):
        span = pl.ds(b * step, step)
        return pltpu.make_async_copy(spread.at[span], own_grad.at[span], out_sem.at[b])

    @pl.loop(0, own // step)
    def _(b):
        span = pl.ds(b * step, step)
        spread[span] = backward[span].astype(bf16)
        out_copy(b).start()

    halo_grad[...] = backward[pl.ds(own, ext - own)].astype(bf16)
    pieces, piece_rows = weight_part.shape[:2]
    for p in range(pieces):
        weight_part[p] = wsum[pl.ds(p * piece_rows, piece_rows), :].astype(bf16)
    bias_part[...] = bsum[...]

    @pl.loop(0, own // step)
    def _(b):
        act_copy(b).wait()
        out_copy(b).wait()


def local_pass(n, tile_row, tile_col, tile_count, features, halo, tiles, cotangent, weight, bias):
    own, edge, width = features.shape
    ext = own + halo.shape[0]
    number = tiles.shape[0]
    chunk = math.gcd(number, CHUNK)
    steps = own // math.gcd(own, 4)
    anywhere = pl.BlockSpec(memory_space=pltpu.HBM)
    smem = pl.BlockSpec(memory_space=pltpu.SMEM)
    vmem = pl.BlockSpec(memory_space=VMEM)
    dma = pltpu.SemaphoreType.DMA
    return pl.pallas_call(
        local_kernel,
        out_shape=(
            jax.ShapeDtypeStruct(features.shape, bf16),
            jax.ShapeDtypeStruct(features.shape, bf16),
            jax.ShapeDtypeStruct(halo.shape, bf16),
            jax.ShapeDtypeStruct((n, width // n, width), bf16),
            jax.ShapeDtypeStruct((1, width), f32),
        ),
        in_specs=[smem] * 3 + [anywhere] * 4 + [vmem] * 2,
        out_specs=(anywhere, anywhere, vmem, vmem, vmem),
        scratch_shapes=[
            VMEM((ext, edge, width), bf16),
            VMEM(tiles.shape, bf16),
            VMEM(features.shape, bf16),
            VMEM(features.shape, bf16),
            VMEM(features.shape, bf16),
            VMEM((own + 1, edge, width), f32),
            VMEM((ext + 1, edge, width), f32),
            VMEM(features.shape, bf16),
            VMEM((width, width), f32),
            VMEM((1, width), f32),
            dma((2,)),
            dma((number // chunk,)),
            dma,
            dma((steps,)),
            dma((steps,)),
        ],
        compiler_params=pltpu.CompilerParams(vmem_limit_bytes=56 * 1024 * 1024),
        name="local_pass",
    )(tile_row, tile_col, tile_count, features, halo, tiles, cotangent, weight, bias)


def return_kernel(
    n, scale, count_ref, chosen_ref, halo_ref, weight_ref, bias_ref, own_hbm,
    out_hbm, wsum_ref, bsum_ref,
    halo_in, weight_in, bias_in, piece, pieces_in, returned, own, hot, out, load_sem, out_sem,
    halo_s, halo_r, weight_s, weight_r, bias_s, bias_r, piece_s, piece_r,
):
    me = lax.axis_index("dom")
    load = pltpu.make_async_copy(own_hbm, own, load_sem)
    load.start()
    barrier = greet(n, me)
    pl.semaphore_wait(barrier, n - 1)
    halo_copy = functools.partial(push, n, me, lambda p: halo_ref.at[p], halo_in, halo_s, halo_r)
    weight_copy = functools.partial(
        push, n, me, lambda p: weight_ref.at[p], weight_in, weight_s, weight_r
    )
    bias_copy = functools.partial(push, n, me, lambda p: bias_ref, bias_in, bias_s, bias_r)
    piece_copy = functools.partial(push, n, me, lambda p: piece, pieces_in, piece_s, piece_r)

    def over(step):
        def turn(i, carry):
            step(i)
            return carry

        lax.fori_loop(1, n, turn, 0)

    def first(i):
        weight_copy(i).start()
        bias_copy(i).start()

    over(first)
    over(lambda i: halo_copy(i).start())
    weight_in[me] = weight_ref[me]
    bias_in[me] = bias_ref[...]
    halo_in[me] = halo_ref[me]
    rows = own.shape[0]
    slots = chosen_ref.shape[1]
    step = math.gcd(rows, 512)
    for c in range(rows // step):
        ids = lax.broadcasted_iota(jnp.int32, (step, slots), 0) + c * step
        hot[pl.ds(c * step, step), :] = jnp.where(ids == chosen_ref[...], 1.0, 0.0).astype(bf16)
    over(lambda i: weight_copy(i).wait())
    piece[...] = (jnp.sum(weight_in[...].astype(f32), axis=0) * scale).astype(bf16)
    over(lambda i: piece_copy(i).start())
    pieces_in[me] = piece[...]
    over(lambda i: bias_copy(i).wait())
    bsum_ref[...] = jnp.sum(bias_in[...], axis=0) * scale
    over(lambda i: halo_copy(i).wait())
    slot_count = halo_in.shape[1]
    for p in range(n):
        returned[pl.ds(p * slot_count, slot_count), :] = live(
            count_ref, p, halo_in[p].astype(f32)
        ).astype(bf16)
    load.wait()
    outs = []
    for c in range(rows // step):
        span = pl.ds(c * step, step)
        collected = jnp.dot(hot[span, :], returned[...], preferred_element_type=f32)
        out[span, :] = (own[span, :].astype(f32) + collected).astype(bf16)
        outs.append(pltpu.make_async_copy(out.at[span], out_hbm.at[span], out_sem.at[c]))
        outs[c].start()
    over(lambda i: piece_copy(i).wait())
    piece_rows = piece.shape[0]
    for p in range(n):
        wsum_ref[pl.ds(p * piece_rows, piece_rows), :] = pieces_in[p].astype(f32)
    for copy in outs:
        copy.wait()


def exchange_return(n, scale, send_count, chosen, halo_grad, weight_part, bias_part, own_grad):
    rows, width = own_grad.shape
    slots = chosen.shape[1]
    vmem = pl.BlockSpec(memory_space=VMEM)
    hbm = pl.BlockSpec(memory_space=pltpu.HBM)
    return pl.pallas_call(
        functools.partial(return_kernel, n, scale),
        out_shape=(
            jax.ShapeDtypeStruct(own_grad.shape, bf16),
            jax.ShapeDtypeStruct((width, width), f32),
            jax.ShapeDtypeStruct((1, width), f32),
        ),
        in_specs=[pl.BlockSpec(memory_space=pltpu.SMEM)] + [vmem] * 4 + [hbm],
        out_specs=(hbm, vmem, vmem),
        scratch_shapes=[
            VMEM(halo_grad.shape, bf16),
            VMEM(weight_part.shape, bf16),
            VMEM((n,) + bias_part.shape, f32),
            VMEM(weight_part.shape[1:], bf16),
            VMEM(weight_part.shape, bf16),
            VMEM((slots, width), bf16),
            VMEM(own_grad.shape, bf16),
            VMEM((rows, slots), bf16),
            VMEM(own_grad.shape, bf16),
            pltpu.SemaphoreType.DMA,
            pltpu.SemaphoreType.DMA((rows // math.gcd(rows, 512),)),
        ]
        + [pltpu.SemaphoreType.DMA((n,))] * 8,
        compiler_params=pltpu.CompilerParams(
            collective_id=1, has_side_effects=True, vmem_limit_bytes=60 * 1024 * 1024
        ),
        name="return_exchange",
    )(send_count, chosen, halo_grad, weight_part, bias_part, own_grad)


def body(
    features, weight, bias_vector, tile_values, tile_row, tile_col, tile_count, send_rows,
    send_count, cotangent,
):
    rows, width = features.shape
    n = lax.axis_size("dom")
    slot_count = send_rows.shape[2]
    edge = tile_values.shape[1]
    own = rows // edge
    slots = n * slot_count
    halo = exchange_gather(n, send_count, send_rows.reshape(slots, 1), features, slot_count)
    blocks = lambda a: a.reshape(-1, edge, width)
    activation, own_grad, halo_grad, weight_part, bias_part = local_pass(
        n, tile_row, tile_col, tile_count, blocks(features), blocks(halo), tile_values,
        blocks(cotangent), weight, bias_vector.reshape(1, width),
    )
    scale = float(rows * n) ** (-0.5)
    grad_features, weight_sum, bias_sum = exchange_return(
        n, scale, send_count, send_rows.reshape(1, slots),
        halo_grad.reshape(n, slot_count, width), weight_part, bias_part,
        own_grad.reshape(rows, width),
    )
    return (activation.reshape(rows, width), grad_features, weight_sum, bias_sum.reshape(width))


def solution(mesh):
    return jax.shard_map(
        body,
        mesh=mesh,
        in_specs=(
            P("dom", None),
            P(),
            P(),
            P("dom", None, None),
            P("dom", None),
            P("dom", None),
            P("dom"),
            P("dom", None, None),
            P("dom", None),
            P("dom", None),
        ),
        out_specs=(P("dom", None), P("dom", None), P(), P()),
        check_vma=False,
    )
```
